32 devices in a mesh: kgrp: 4 (over x, core), tile: 8 (over z, y).
Axes of the slice: x: 2, y: 2, z: 4, core: 2. Of those that a mesh axis runs over, the one named last changes fastest.
Arguments:
- mask_spectrum: float32 [32, 2, 512, 512], P(('kgrp', 'tile')), may hold values from -6 to 6
- kernels: float32 [8, 2, 512, 512], P('kgrp', None, 'tile'), may hold values from -6 to 6
- owner_table: int32 [4], replicated, may hold values from 0 to 7
- step_weight: float32 [4], replicated, may hold values from 0.25 to 1
Outputs:
- intensity: float32 [32, 512, 512], P(('kgrp', 'tile'))
The draws below stay inside these ranges and needn't reach their ends.
Inputs may be any that keep to these rules, and one draw needn't show every extreme that they name: `owner_table`: kernel indices, possibly repeated across steps.
All inputs are finite; a program needn't handle non-finite values.
Results may differ from the reference program's by a relative error of at most 0.0001.
Values sent between devices are 32-bit elements; how exact they have to be, the bound alone decides.
A program may use at most 128 MiB of HBM per device.

```python
import math
import jax
import jax.numpy as jnp

KS = 512
STEPS = 4
KERNELS = 8
TILES = 32


def with_ends(entries, rng, least, high):
    longest = entries.shape.index(max(entries.shape))
    spots = []
    for shift in (0, 1):
        where = [jax.random.randint(jax.random.fold_in(rng, axis), (), 0, length) for axis, length in enumerate(entries.shape)]
        where[longest] = (where[longest] + shift) % entries.shape[longest]
        spots.append(tuple(where))
    return entries.at[spots[0]].set(least).at[spots[1]].set(high)


def shard_levels(rng, shape, cuts, least, largest):
    level = 1.0
    for position, parts in cuts:
        draws = jax.random.uniform(jax.random.fold_in(jax.random.fold_in(rng, 6), position), (parts,), jnp.float32, least / len(cuts), largest / len(cuts))
        level = level * jnp.repeat(jnp.exp(draws), shape[position] // parts).reshape((-1,) + (1,) * (len(shape) - 1 - position))
    return level


def bell_draw(own_key, shape, deviation, reach, pieces=(), kind=jnp.bfloat16):
    entries = deviation * jax.random.normal(own_key, shape, jnp.float32)
    if pieces:
        entries = entries * shard_levels(own_key, shape, pieces, -0.22, 0.18)
    return jnp.clip(entries, -reach, reach).astype(kind)


def setup_inputs(seed: int = 0) -> dict:
    key_of = jax.random.split(jax.random.key(seed), 5)
    mask_spectrum = bell_draw(key_of[0], (TILES, 2, KS, KS), 0.7, 6.0, ((0, 32),), jnp.float32)
    kernels = bell_draw(key_of[1], (KERNELS, 2, KS, KS), 0.7, 6.0, ((0, 4), (2, 8)), jnp.float32)
    owner_table = with_ends(jax.random.randint(key_of[2], (STEPS,), 0, KERNELS), jax.random.fold_in(key_of[2], 1), 0, KERNELS - 1).astype(jnp.int32)
    step_weight = jnp.clip(jnp.exp(jax.random.uniform(key_of[3], (STEPS,), jnp.float32, math.log(0.25), math.log(1.0))), 0.25, 1.0)
    return {"mask_spectrum": mask_spectrum, "kernels": kernels, "owner_table": owner_table, "step_weight": step_weight}


def reference(mask_spectrum, kernels, owner_table, step_weight):
    mask_field = mask_spectrum[:, 0] + 1j * mask_spectrum[:, 1]
    intensity = jnp.zeros_like(mask_spectrum[:, 0])
    for step in range(STEPS):
        kernel_pick = kernels[owner_table[step]]
        spectrum = mask_field * (kernel_pick[0] + 1j * kernel_pick[1])[None]
        aerial_field = jnp.fft.ifft2(spectrum, norm="ortho")
        power = jnp.real(aerial_field) ** 2 + jnp.imag(aerial_field) ** 2
        intensity = intensity + step_weight[step] * power.astype(intensity.dtype)
    return intensity
```

```python
import functools
import math

import jax
import jax.numpy as jnp
import ml_dtypes
import numpy as np
from jax import lax
from jax.experimental import pallas as pl
from jax.experimental.pallas import tpu as pltpu
from jax.sharding import PartitionSpec as P

MESH = pl.DeviceIdType.MESH
BF = jnp.bfloat16
F32 = jnp.float32


def split_np(x):
    hi = x.astype(np.float32).astype(ml_dtypes.bfloat16)
    lo = (x - hi.astype(np.float64)).astype(np.float32).astype(ml_dtypes.bfloat16)
    return hi, lo


def tables(n, radix):
    m = n // radix
    a = np.arange(m)
    rows = []
    for r in range(radix):
        phase = (a[:, None] * (r + radix * a[None, :])) % n * (2.0 * math.pi / n)
        c, s = np.cos(phase) / math.sqrt(n), np.sin(phase) / math.sqrt(n)
        rows.append(np.block([[c, s], [-s, c]]))
    b = np.stack(rows)
    bh, bl = split_np(b)
    row = np.concatenate([bh, bl], axis=1)
    col = np.concatenate([bh.transpose(0, 2, 1), bl.transpose(0, 2, 1)], axis=2)
    return row, col


def split(x):
    hi = x.astype(BF)
    return hi, (x - hi.astype(F32)).astype(BF)


def radix4(re, im):
    ar, ai, br, bi = re[0] + re[2], im[0] + im[2], re[0] - re[2], im[0] - im[2]
    cr, ci, dr, di = re[1] + re[3], im[1] + im[3], re[1] - re[3], im[1] - im[3]
    return [(ar + cr, ai + ci), (br - di, bi + dr), (ar - cr, ai - ci), (br + di, bi - dr)]


def kernel(dims, owner_ref, weight_ref, mask_hbm, kern_hbm, rowt_hbm, colt_hbm, out_ref,
           held, cand, mask, rowt, colt, lane_perm, stage, field, cols, total, blocks,
           z_send, z_recv, x_send, x_recv, y_send, y_recv, d_send, d_recv,
           c_send, c_recv, k_send, k_recv, loc):
    steps, groups, nk, nz, rows, n, m = dims
    g = lax.axis_index("kgrp")
    t = lax.axis_index("tile")
    x, c = g // 2, g % 2
    xo, co = 1 - x, 1 - c
    z, y = t // 2, t % 2
    yo = 1 - y
    x_peer, c_peer = {"kgrp": 2 * xo + c}, {"kgrp": 2 * x + co}
    y_peer = {"tile": 2 * z + yo}
    d_peer = {"kgrp": 2 * (x * (1 - c) + xo * c) + c, "tile": 2 * z + yo * (1 - c) + y * c}
    d_q = 2 * (xo * (1 - c) + x * c) + c
    d_y = y * (1 - c) + yo * c

    loads = [
        pltpu.make_async_copy(kern_hbm.at[:, :, :, pl.ds(pl.multiple_of(g * m, m), m)], cand.at[pl.ds(g * nk, nk)], loc.at[0]),
        pltpu.make_async_copy(mask_hbm, mask, loc.at[1]),
        pltpu.make_async_copy(rowt_hbm, rowt, loc.at[2]),
        pltpu.make_async_copy(colt_hbm, colt, loc.at[3]),
    ]
    for load in loads:
        load.start()

    barrier = pltpu.get_barrier_semaphore()
    for d in range(1, groups):
        pl.semaphore_signal(barrier, inc=1, device_id={"kgrp": (g + d) % groups}, device_id_type=MESH)
    pl.semaphore_signal(barrier, inc=1, device_id=y_peer, device_id_type=MESH)
    for d in range(1, nz):
        pl.semaphore_signal(barrier, inc=1, device_id={"tile": 2 * ((z + d) % nz) + y}, device_id_type=MESH)
    pl.semaphore_wait(barrier, groups + nz - 1)

    sent = []

    def send(src, dst, send_sem, recv_sem, device):
        copy = pltpu.make_async_remote_copy(src_ref=src, dst_ref=dst, send_sem=send_sem, recv_sem=recv_sem,
                                            device_id=device, device_id_type=MESH)
        copy.start()
        sent.append(copy)

    def arrive(ref, recv_sem):
        pltpu.make_async_remote_copy(src_ref=ref, dst_ref=ref, send_sem=recv_sem, recv_sem=recv_sem,
                                     device_id=c_peer, device_id_type=MESH).wait_recv()

    for d in range(1, groups):
        peer = (g + d) % groups
        send(kern_hbm.at[:, :, :, pl.ds(pl.multiple_of(peer * m, m), m)], cand.at[pl.ds(g * nk, nk)],
             k_send.at[d - 1], k_recv.at[d - 1], {"kgrp": peer})

    src_lane = lax.broadcasted_iota(jnp.int32, (n, n), 0)
    dst_lane = lax.broadcasted_iota(jnp.int32, (n, n), 1)
    radix = n // m
    lane_perm[...] = jnp.where((src_lane % m) * radix + src_lane // m == dst_lane, 1.0, 0.0).astype(BF)

    loads[0].wait()
    for d in range(1, groups):
        arrive(cand.at[pl.ds(((g + groups - d) % groups) * nk, nk)], k_recv.at[d - 1])
    for s in range(steps):
        held[s, g, :, z, y] = cand[owner_ref[s]]

    def near(d):
        return (z + d) % nz

    def piece(s, q, zz, yy):
        return held.at[s, q, :, zz, yy]

    def line(s, q, yy):
        return held.at[s, q, :, :, yy]

    def cross(s, d):
        own = piece(s, g, near(d), y)
        send(own, own, x_send.at[s, d], x_recv.at[s, d], x_peer)
        send(own, own, y_send.at[s, d], y_recv.at[s, d], y_peer)

    def to_core(s, kind, q, yy):
        send(line(s, q, yy), line(s, q, yy), c_send.at[s, kind], c_recv.at[s, kind], c_peer)

    def gather_z(s):
        for d in range(1, nz):
            arrive(piece(s, g, near(nz - d), y), z_recv.at[s, d])
            cross(s, nz - d)
        to_core(s, 0, g, y)

    def gather_xy(s):
        for d in [0] + [nz - d for d in range(1, nz)]:
            arrive(piece(s, 2 * xo + c, near(d), y), x_recv.at[s, d])
            arrive(piece(s, g, near(d), yo), y_recv.at[s, d])
            turned = piece(s, d_q, near(d), d_y)
            send(turned, turned, d_send.at[s, d], d_recv.at[s, d], d_peer)
        to_core(s, 1, 2 * xo + c, y)
        to_core(s, 2, g, yo)

    def gather_rest(s):
        for d in range(nz):
            arrive(piece(s, 2 * xo + c, near(d), yo), d_recv.at[s, d])
        to_core(s, 3, 2 * xo + c, yo)
        for kind, (q, yy) in enumerate([(2 * x + co, y), (2 * xo + co, y), (2 * x + co, yo), (2 * xo + co, yo)]):
            arrive(line(s, q, yy), c_recv.at[s, kind])

    def compute(s):
        @pl.loop(0, 2 * nz)
        def _(i):
            at = pl.ds(pl.multiple_of(i * rows, rows), rows)
            re, im = [], []
            for q in range(groups):
                kr, ki = held[s, q, 0, i // 2, i % 2], held[s, q, 1, i // 2, i % 2]
                mr, mi = mask[0, at, q * m:(q + 1) * m], mask[1, at, q * m:(q + 1) * m]
                re.append(mr * kr - mi * ki)
                im.append(mr * ki + mi * kr)
            for r, (pr, pi) in enumerate(radix4(re, im)):
                for p, part in enumerate((pr, pi)):
                    hi, lo = split(part)
                    stage[r, at, p * m:(p + 1) * m] = hi
                    stage[r, at, (2 + p) * m:(3 + p) * m] = lo

        for r in range(radix):
            hi, lo = stage[r, :, :2 * m], stage[r, :, 2 * m:]
            th, tl = rowt[r, :2 * m], rowt[r, 2 * m:]
            field[r] = jnp.dot(jnp.concatenate([hi, lo, hi], 1), jnp.concatenate([th, th, tl], 0),
                               preferred_element_type=F32)

        half = m // 4
        for ry in range(radix):
            @pl.loop(0, 4)
            def _(i):
                base = pl.multiple_of(i * half, half)
                re = [field[ry, pl.ds(k * m + base, half), :m] for k in range(radix)]
                im = [field[ry, pl.ds(k * m + base, half), m:] for k in range(radix)]
                for rx, parts in enumerate(radix4(re, im)):
                    for p, part in enumerate(parts):
                        hi, lo = split(part)
                        cols[rx, pl.ds(p * m + base, half), ry * m:(ry + 1) * m] = hi
                        cols[rx, pl.ds((2 + p) * m + base, half), ry * m:(ry + 1) * m] = lo

        for rx in range(radix):
            hi, lo = cols[rx, :2 * m], cols[rx, 2 * m:]
            th, tl = colt[rx, :, :2 * m], colt[rx, :, 2 * m:]
            done = jnp.dot(jnp.concatenate([th, th, tl], 1), jnp.concatenate([hi, lo, hi], 0),
                           preferred_element_type=F32)
            power = (done[:m] * done[:m] + done[m:] * done[m:]) * weight_ref[s]
            if s == 0:
                total[rx] = power
            else:
                total[rx] += power

    for s in range(steps):
        own = piece(s, g, z, y)
        for d in range(1, nz):
            send(own, own, z_send.at[s, d], z_recv.at[s, d], {"tile": 2 * near(d) + y})
        cross(s, 0)
    for load in loads[1:]:
        load.wait()
    gather_z(0)
    for s in range(steps):
        if s + 1 < steps:
            gather_z(s + 1)
        gather_xy(s)
        if s:
            gather_rest(s - 1)
            compute(s - 1)
    gather_rest(steps - 1)
    compute(steps - 1)

    for rx in range(radix):
        hi, lo = split(total[rx])
        perm = lane_perm[...]
        image = jnp.dot(jnp.concatenate([hi, lo], 1), jnp.concatenate([perm, perm], 0), preferred_element_type=F32)
        for q in range(radix):
            blocks[q, pl.ds(rx, m, stride=radix), :] = image[:, q * m:(q + 1) * m]
    for q in range(radix):
        out_ref[:, q * m:(q + 1) * m] = blocks[q]
    for copy in sent:
        copy.wait_send()


def local(mesh_shape, mask_spectrum, kernels, owner_table, step_weight):
    groups, tiles = mesh_shape
    nk, _, rows, n = kernels.shape
    steps = owner_table.shape[0]
    m = n // groups
    radix = groups
    nz = tiles // 2
    rowt, colt = tables(n, radix)
    dma = pltpu.SemaphoreType.DMA
    any_spec = pl.BlockSpec(memory_space=pl.ANY)
    smem = pl.BlockSpec(memory_space=pltpu.SMEM)
    out = pl.pallas_call(
        functools.partial(kernel, (steps, groups, nk, nz, rows, n, m)),
        out_shape=jax.ShapeDtypeStruct((n, n), F32),
        in_specs=[smem, smem, any_spec, any_spec, any_spec, any_spec],
        out_specs=pl.BlockSpec(memory_space=pltpu.VMEM),
        scratch_shapes=[
            pltpu.VMEM((steps, groups, 2, nz, 2, rows, m), F32),
            pltpu.VMEM((groups * nk, 2, rows, m), F32),
            pltpu.VMEM((2, n, n), F32),
            pltpu.VMEM(rowt.shape, BF),
            pltpu.VMEM(colt.shape, BF),
            pltpu.VMEM((n, n), BF),
            pltpu.VMEM((radix, n, 4 * m), BF),
            pltpu.VMEM((radix, n, 2 * m), F32),
            pltpu.VMEM((radix, 4 * m, n), BF),
            pltpu.VMEM((radix, m, n), F32),
            pltpu.VMEM((radix, n, m), F32),
        ] + [dma((steps, nz))] * 8 + [dma((steps, 4))] * 2 + [dma((groups - 1,))] * 2 + [dma((4,))],
        compiler_params=pltpu.CompilerParams(collective_id=0, has_side_effects=True, vmem_limit_bytes=62 * 1024 * 1024),
    )(owner_table, step_weight, mask_spectrum[0], kernels, jnp.asarray(rowt), jnp.asarray(colt))
    return out[None]


def solution(mesh):
    in_specs = (P(("kgrp", "tile"), None, None, None), P("kgrp", None, "tile", None), P(), P())
    out_specs = P(("kgrp", "tile"), None, None)
    body = functools.partial(local, (mesh.shape["kgrp"], mesh.shape["tile"]))
    return jax.shard_map(body, mesh=mesh, in_specs=in_specs, out_specs=out_specs, check_vma=False)
```

```python
import functools
import math

import jax
import jax.numpy as jnp
import ml_dtypes
import numpy as np
from jax import lax
from jax.experimental import pallas as pl
from jax.experimental.pallas import tpu as pltpu
from jax.sharding import PartitionSpec as P

MESH = pl.DeviceIdType.MESH
BF = jnp.bfloat16
F32 = jnp.float32


def split_np(x):
    hi = x.astype(np.float32).astype(ml_dtypes.bfloat16)
    lo = (x - hi.astype(np.float64)).astype(np.float32).astype(ml_dtypes.bfloat16)
    return hi, lo


def tables(n, radix):
    m = n // radix
    a = np.arange(m)
    rows = []
    for r in range(radix):
        phase = (a[:, None] * (r + radix * a[None, :])) % n * (2.0 * math.pi / n)
        c, s = np.cos(phase) / math.sqrt(n), np.sin(phase) / math.sqrt(n)
        rows.append(np.block([[c, s], [-s, c]]))
    b = np.stack(rows)
    bh, bl = split_np(b)
    row = np.concatenate([bh, bl], axis=1)
    col = np.concatenate([bh.transpose(0, 2, 1), bl.transpose(0, 2, 1)], axis=2)
    return row, col


def split(x):
    hi = x.astype(BF)
    return hi, (x - hi.astype(F32)).astype(BF)


def radix4(re, im):
    ar, ai, br, bi = re[0] + re[2], im[0] + im[2], re[0] - re[2], im[0] - im[2]
    cr, ci, dr, di = re[1] + re[3], im[1] + im[3], re[1] - re[3], im[1] - im[3]
    return [(ar + cr, ai + ci), (br - di, bi + dr), (ar - cr, ai - ci), (br + di, bi - dr)]


def kernel(dims, owner_ref, weight_ref, mask_hbm, kern_hbm, rowt_hbm, colt_hbm, total,
           held, cand, mask, rowt, colt, stage, field, cols,
           z_send, z_recv, x_send, x_recv, y_send, y_recv, d_send, d_recv,
           c_send, c_recv, k_send, k_recv, loc):
    steps, groups, nk, nz, rows, n, m = dims
    g = lax.axis_index("kgrp")
    t = lax.axis_index("tile")
    x, c = g // 2, g % 2
    xo, co = 1 - x, 1 - c
    z, y = t // 2, t % 2
    yo = 1 - y
    x_peer, c_peer = {"kgrp": 2 * xo + c}, {"kgrp": 2 * x + co}
    y_peer = {"tile": 2 * z + yo}
    d_peer = {"kgrp": 2 * (x * (1 - c) + xo * c) + c, "tile": 2 * z + yo * (1 - c) + y * c}
    d_q = 2 * (xo * (1 - c) + x * c) + c
    d_y = y * (1 - c) + yo * c

    loads = [
        pltpu.make_async_copy(kern_hbm.at[:, :, :, pl.ds(pl.multiple_of(g * m, m), m)], cand.at[pl.ds(g * nk, nk)], loc.at[0]),
        pltpu.make_async_copy(mask_hbm, mask, loc.at[1]),
        pltpu.make_async_copy(rowt_hbm, rowt, loc.at[2]),
        pltpu.make_async_copy(colt_hbm, colt, loc.at[3]),
    ]
    for load in loads:
        load.start()

    barrier = pltpu.get_barrier_semaphore()
    for d in range(1, groups):
        pl.semaphore_signal(barrier, inc=1, device_id={"kgrp": (g + d) % groups}, device_id_type=MESH)
    pl.semaphore_signal(barrier, inc=1, device_id=y_peer, device_id_type=MESH)
    for d in range(1, nz):
        pl.semaphore_signal(barrier, inc=1, device_id={"tile": 2 * ((z + d) % nz) + y}, device_id_type=MESH)
    pl.semaphore_wait(barrier, groups + nz - 1)

    sent = []

    def send(src, dst, send_sem, recv_sem, device):
        copy = pltpu.make_async_remote_copy(src_ref=src, dst_ref=dst, send_sem=send_sem, recv_sem=recv_sem,
                                            device_id=device, device_id_type=MESH)
        copy.start()
        sent.append(copy)

    def arrive(ref, recv_sem):
        pltpu.make_async_remote_copy(src_ref=ref, dst_ref=ref, send_sem=recv_sem, recv_sem=recv_sem,
                                     device_id=c_peer, device_id_type=MESH).wait_recv()

    for d in range(1, groups):
        peer = (g + d) % groups
        send(kern_hbm.at[:, :, :, pl.ds(pl.multiple_of(peer * m, m), m)], cand.at[pl.ds(g * nk, nk)],
             k_send.at[d - 1], k_recv.at[d - 1], {"kgrp": peer})

    radix = n // m
    loads[0].wait()
    for d in range(1, groups):
        arrive(cand.at[pl.ds(((g + groups - d) % groups) * nk, nk)], k_recv.at[d - 1])
    for s in range(steps):
        held[s, g, :, z, y] = cand[owner_ref[s]]

    def near(d):
        return (z + d) % nz

    def piece(s, q, zz, yy):
        return held.at[s, q, :, zz, yy]

    def line(s, q, yy):
        return held.at[s, q, :, :, yy]

    def cross(s, d):
        own = piece(s, g, near(d), y)
        send(own, own, x_send.at[s, d], x_recv.at[s, d], x_peer)
        send(own, own, y_send.at[s, d], y_recv.at[s, d], y_peer)

    def to_core(s, kind, q, yy):
        send(line(s, q, yy), line(s, q, yy), c_send.at[s, kind], c_recv.at[s, kind], c_peer)

    def gather_z(s):
        for d in range(1, nz):
            arrive(piece(s, g, near(nz - d), y), z_recv.at[s, d])
            cross(s, nz - d)
        to_core(s, 0, g, y)

    def gather_xy(s):
        for d in [0] + [nz - d for d in range(1, nz)]:
            arrive(piece(s, 2 * xo + c, near(d), y), x_recv.at[s, d])
            arrive(piece(s, g, near(d), yo), y_recv.at[s, d])
            turned = piece(s, d_q, near(d), d_y)
            send(turned, turned, d_send.at[s, d], d_recv.at[s, d], d_peer)
        to_core(s, 1, 2 * xo + c, y)
        to_core(s, 2, g, yo)

    def gather_rest(s):
        for d in range(nz):
            arrive(piece(s, 2 * xo + c, near(d), yo), d_recv.at[s, d])
        to_core(s, 3, 2 * xo + c, yo)
        for kind, (q, yy) in enumerate([(2 * x + co, y), (2 * xo + co, y), (2 * x + co, yo), (2 * xo + co, yo)]):
            arrive(line(s, q, yy), c_recv.at[s, kind])

    def compute(s):
        @pl.loop(0, 2 * nz)
        def _(i):
            at = pl.ds(pl.multiple_of(i * rows, rows), rows)
            re, im = [], []
            for q in range(groups):
                kr, ki = held[s, q, 0, i // 2, i % 2], held[s, q, 1, i // 2, i % 2]
                mr, mi = mask[0, at, q * m:(q + 1) * m], mask[1, at, q * m:(q + 1) * m]
                re.append(mr * kr - mi * ki)
                im.append(mr * ki + mi * kr)
            for r, (pr, pi) in enumerate(radix4(re, im)):
                for p, part in enumerate((pr, pi)):
                    hi, lo = split(part)
                    stage[r, at, p * m:(p + 1) * m] = hi
                    stage[r, at, (2 + p) * m:(3 + p) * m] = lo

        for r in range(radix):
            hi, lo = stage[r, :, :2 * m], stage[r, :, 2 * m:]
            th, tl = rowt[r, :2 * m], rowt[r, 2 * m:]
            field[r] = jnp.dot(jnp.concatenate([hi, lo, hi], 1), jnp.concatenate([th, th, tl], 0),
                               preferred_element_type=F32)

        half = m // 4
        for ry in range(radix):
            @pl.loop(0, 4)
            def _(i):
                base = pl.multiple_of(i * half, half)
                re = [field[ry, pl.ds(k * m + base, half), :m] for k in range(radix)]
                im = [field[ry, pl.ds(k * m + base, half), m:] for k in range(radix)]
                for rx, parts in enumerate(radix4(re, im)):
                    for p, part in enumerate(parts):
                        hi, lo = split(part)
                        cols[rx, pl.ds(p * m + base, half), ry * m:(ry + 1) * m] = hi
                        cols[rx, pl.ds((2 + p) * m + base, half), ry * m:(ry + 1) * m] = lo

        for rx in range(radix):
            hi, lo = cols[rx, :2 * m], cols[rx, 2 * m:]
            th, tl = colt[rx, :, :2 * m], colt[rx, :, 2 * m:]
            done = jnp.dot(jnp.concatenate([th, th, tl], 1), jnp.concatenate([hi, lo, hi], 0),
                           preferred_element_type=F32)
            power = (done[:m] * done[:m] + done[m:] * done[m:]) * weight_ref[s]
            if s == 0:
                total[rx] = power
            else:
                total[rx] += power

    for s in range(steps):
        own = piece(s, g, z, y)
        for d in range(1, nz):
            send(own, own, z_send.at[s, d], z_recv.at[s, d], {"tile": 2 * near(d) + y})
        cross(s, 0)
    for load in loads[1:]:
        load.wait()
    gather_z(0)
    for s in range(steps):
        if s + 1 < steps:
            gather_z(s + 1)
        gather_xy(s)
        if s:
            gather_rest(s - 1)
            compute(s - 1)
    gather_rest(steps - 1)
    compute(steps - 1)

    for copy in sent:
        copy.wait_send()


def order(dims, total, out_ref, lane_perm, blocks):
    radix, m, n = dims
    part = total.shape[1]

    @pl.when(pl.program_id(0) == 0)
    def _():
        src_lane = lax.broadcasted_iota(jnp.int32, (n, n), 0)
        dst_lane = lax.broadcasted_iota(jnp.int32, (n, n), 1)
        lane_perm[...] = jnp.where((src_lane % m) * radix + src_lane // m == dst_lane, 1.0, 0.0).astype(BF)

    hi, lo = split(total[...].reshape(radix * part, n))
    perm = lane_perm[...]
    image = jnp.dot(jnp.concatenate([hi, lo], 1), jnp.concatenate([perm, perm], 0), preferred_element_type=F32)
    for q in range(radix):
        for rx in range(radix):
            blocks[q, pl.ds(rx, part, stride=radix), :] = image[rx * part:(rx + 1) * part, q * m:(q + 1) * m]
    for q in range(radix):
        out_ref[:, q * m:(q + 1) * m] = blocks[q]


def local(mesh_shape, mask_spectrum, kernels, owner_table, step_weight):
    groups, tiles = mesh_shape
    nk, _, rows, n = kernels.shape
    steps = owner_table.shape[0]
    m = n // groups
    radix = groups
    nz = tiles // 2
    rowt, colt = tables(n, radix)
    dma = pltpu.SemaphoreType.DMA
    any_spec = pl.BlockSpec(memory_space=pl.ANY)
    smem = pl.BlockSpec(memory_space=pltpu.SMEM)
    total = pl.pallas_call(
        functools.partial(kernel, (steps, groups, nk, nz, rows, n, m)),
        out_shape=jax.ShapeDtypeStruct((radix, m, n), F32),
        in_specs=[smem, smem, any_spec, any_spec, any_spec, any_spec],
        out_specs=pl.BlockSpec(memory_space=pltpu.VMEM),
        scratch_shapes=[
            pltpu.VMEM((steps, groups, 2, nz, 2, rows, m), F32),
            pltpu.VMEM((groups * nk, 2, rows, m), F32),
            pltpu.VMEM((2, n, n), F32),
            pltpu.VMEM(rowt.shape, BF),
            pltpu.VMEM(colt.shape, BF),
            pltpu.VMEM((radix, n, 4 * m), BF),
            pltpu.VMEM((radix, n, 2 * m), F32),
            pltpu.VMEM((radix, 4 * m, n), BF),
        ] + [dma((steps, nz))] * 8 + [dma((steps, 4))] * 2 + [dma((groups - 1,))] * 2 + [dma((4,))],
        compiler_params=pltpu.CompilerParams(collective_id=0, has_side_effects=True, vmem_limit_bytes=62 * 1024 * 1024),
    )(owner_table, step_weight, mask_spectrum[0], kernels, jnp.asarray(rowt), jnp.asarray(colt))
    part = m // 4
    out = pl.pallas_call(
        functools.partial(order, (radix, m, n)),
        grid=(4,),
        out_shape=jax.ShapeDtypeStruct((n, n), F32),
        in_specs=[pl.BlockSpec((radix, part, n), lambda i: (0, i, 0))],
        out_specs=pl.BlockSpec((radix * part, n), lambda i: (i, 0)),
        scratch_shapes=[pltpu.VMEM((n, n), BF), pltpu.VMEM((radix, radix * part, m), F32)],
    )(total)
    return out[None]


def solution(mesh):
    in_specs = (P(("kgrp", "tile"), None, None, None), P("kgrp", None, "tile", None), P(), P())
    out_specs = P(("kgrp", "tile"), None, None)
    body = functools.partial(local, (mesh.shape["kgrp"], mesh.shape["tile"]))
    return jax.shard_map(body, mesh=mesh, in_specs=in_specs, out_specs=out_specs, check_vma=False)
```

```python
import functools
import math

import jax
import jax.numpy as jnp
import ml_dtypes
import numpy as np
from jax import lax
from jax.experimental import pallas as pl
from jax.experimental.pallas import tpu as pltpu
from jax.sharding import PartitionSpec as P

MESH = pl.DeviceIdType.MESH
BF = jnp.bfloat16
F32 = jnp.float32


def split_np(x):
    hi = x.astype(np.float32).astype(ml_dtypes.bfloat16)
    lo = (x - hi.astype(np.float64)).astype(np.float32).astype(ml_dtypes.bfloat16)
    return hi, lo


def tables(n, radix):
    m = n // radix
    a = np.arange(m)
    rows = []
    for r in range(radix):
        phase = (a[:, None] * (r + radix * a[None, :])) % n * (2.0 * math.pi / n)
        c, s = np.cos(phase) / math.sqrt(n), np.sin(phase) / math.sqrt(n)
        rows.append(np.block([[c, s], [-s, c]]))
    b = np.stack(rows)
    bh, bl = split_np(b)
    row = np.concatenate([bh, bl], axis=1)
    col = np.concatenate([bh.transpose(0, 2, 1), bl.transpose(0, 2, 1)], axis=2)
    return row, col


def split(x):
    hi = x.astype(BF)
    return hi, (x - hi.astype(F32)).astype(BF)


def radix4(re, im):
    ar, ai, br, bi = re[0] + re[2], im[0] + im[2], re[0] - re[2], im[0] - im[2]
    cr, ci, dr, di = re[1] + re[3], im[1] + im[3], re[1] - re[3], im[1] - im[3]
    return [(ar + cr, ai + ci), (br - di, bi + dr), (ar - cr, ai - ci), (br + di, bi - dr)]


def kernel(dims, owner_ref, weight_ref, mask_hbm, kern_hbm, rowt_hbm, colt_hbm, out_ref,
           held, cand, mask, rowt, colt, lane_perm, stage, field, cols, total, blocks,
           z_send, z_recv, x_send, x_recv, y_send, y_recv, d_send, d_recv,
           c_send, c_recv, k_send, k_recv, loc):
    steps, groups, nk, nz, rows, n, m = dims
    g = lax.axis_index("kgrp")
    t = lax.axis_index("tile")
    x, c = g // 2, g % 2
    xo, co = 1 - x, 1 - c
    z, y = t // 2, t % 2
    yo = 1 - y
    x_peer, c_peer = {"kgrp": 2 * xo + c}, {"kgrp": 2 * x + co}
    y_peer = {"tile": 2 * z + yo}
    d_peer = {"kgrp": 2 * (x * (1 - c) + xo * c) + c, "tile": 2 * z + yo * (1 - c) + y * c}
    d_q = 2 * (xo * (1 - c) + x * c) + c
    d_y = y * (1 - c) + yo * c

    loads = [
        pltpu.make_async_copy(kern_hbm.at[:, :, :, pl.ds(pl.multiple_of(g * m, m), m)], cand.at[pl.ds(g * nk, nk)], loc.at[0]),
        pltpu.make_async_copy(mask_hbm, mask, loc.at[1]),
        pltpu.make_async_copy(rowt_hbm, rowt, loc.at[2]),
        pltpu.make_async_copy(colt_hbm, colt, loc.at[3]),
    ]
    for load in loads:
        load.start()

    barrier = pltpu.get_barrier_semaphore()
    for d in range(1, groups):
        pl.semaphore_signal(barrier, inc=1, device_id={"kgrp": (g + d) % groups}, device_id_type=MESH)
    pl.semaphore_signal(barrier, inc=1, device_id=y_peer, device_id_type=MESH)
    for d in range(1, nz):
        pl.semaphore_signal(barrier, inc=1, device_id={"tile": 2 * ((z + d) % nz) + y}, device_id_type=MESH)
    pl.semaphore_wait(barrier, groups + nz - 1)

    sent = []

    def send(src, dst, send_sem, recv_sem, device):
        copy = pltpu.make_async_remote_copy(src_ref=src, dst_ref=dst, send_sem=send_sem, recv_sem=recv_sem,
                                            device_id=device, device_id_type=MESH)
        copy.start()
        sent.append(copy)

    def arrive(ref, recv_sem):
        pltpu.make_async_remote_copy(src_ref=ref, dst_ref=ref, send_sem=recv_sem, recv_sem=recv_sem,
                                     device_id=c_peer, device_id_type=MESH).wait_recv()

    for d in range(1, groups):
        peer = (g + d) % groups
        send(kern_hbm.at[:, :, :, pl.ds(pl.multiple_of(peer * m, m), m)], cand.at[pl.ds(g * nk, nk)],
             k_send.at[d - 1], k_recv.at[d - 1], {"kgrp": peer})

    src_lane = lax.broadcasted_iota(jnp.int32, (n, n), 0)
    dst_lane = lax.broadcasted_iota(jnp.int32, (n, n), 1)
    radix = n // m
    lane_perm[...] = jnp.where((src_lane % m) * radix + src_lane // m == dst_lane, 1.0, 0.0).astype(BF)

    loads[0].wait()
    for d in range(1, groups):
        arrive(cand.at[pl.ds(((g + groups - d) % groups) * nk, nk)], k_recv.at[d - 1])
    for s in range(steps):
        held[s, g, :, z, y] = cand[owner_ref[s]]

    def near(d):
        return (z + d) % nz

    def piece(s, q, zz, yy):
        return held.at[s, q, :, zz, yy]

    def line(s, q, yy):
        return held.at[s, q, :, :, yy]

    def cross(s, d):
        own = piece(s, g, near(d), y)
        send(own, own, x_send.at[s, d], x_recv.at[s, d], x_peer)
        send(own, own, y_send.at[s, d], y_recv.at[s, d], y_peer)

    def to_core(s, kind, q, yy):
        send(line(s, q, yy), line(s, q, yy), c_send.at[s, kind], c_recv.at[s, kind], c_peer)

    def gather_z(s):
        for d in range(1, nz):
            arrive(piece(s, g, near(nz - d), y), z_recv.at[s, d])
            cross(s, nz - d)
        to_core(s, 0, g, y)

    def gather_xy(s):
        for d in [0] + [nz - d for d in range(1, nz)]:
            arrive(piece(s, 2 * xo + c, near(d), y), x_recv.at[s, d])
            arrive(piece(s, g, near(d), yo), y_recv.at[s, d])
            turned = piece(s, d_q, near(d), d_y)
            send(turned, turned, d_send.at[s, d], d_recv.at[s, d], d_peer)
        to_core(s, 1, 2 * xo + c, y)
        to_core(s, 2, g, yo)

    def gather_turned(s):
        for d in range(nz):
            arrive(piece(s, 2 * xo + c, near(d), yo), d_recv.at[s, d])
        to_core(s, 3, 2 * xo + c, yo)

    def rows_in(s, yy):
        for kind in (0, 1) if yy is y else (2, 3):
            arrive(line(s, 2 * x + co if kind % 2 == 0 else 2 * xo + co, yy), c_recv.at[s, kind])

        @pl.loop(0, nz)
        def _(zi):
            i = 2 * zi + yy
            at = pl.ds(pl.multiple_of(i * rows, rows), rows)
            re, im = [], []
            for q in range(groups):
                kr, ki = held[s, q, 0, zi, yy], held[s, q, 1, zi, yy]
                mr, mi = mask[0, at, q * m:(q + 1) * m], mask[1, at, q * m:(q + 1) * m]
                re.append(mr * kr - mi * ki)
                im.append(mr * ki + mi * kr)
            for r, (pr, pi) in enumerate(radix4(re, im)):
                for p, part in enumerate((pr, pi)):
                    hi, lo = split(part)
                    stage[r, at, p * m:(p + 1) * m] = hi
                    stage[r, at, (2 + p) * m:(3 + p) * m] = lo

    def compute(s):
        gather_turned(s)
        rows_in(s, y)
        rows_in(s, yo)
        for r in range(radix):
            hi, lo = stage[r, :, :2 * m], stage[r, :, 2 * m:]
            th, tl = rowt[r, :2 * m], rowt[r, 2 * m:]
            field[r] = jnp.dot(jnp.concatenate([hi, lo, hi], 1), jnp.concatenate([th, th, tl], 0),
                               preferred_element_type=F32)

        half = m // 4
        for ry in range(radix):
            @pl.loop(0, 4)
            def _(i):
                base = pl.multiple_of(i * half, half)
                re = [field[ry, pl.ds(k * m + base, half), :m] for k in range(radix)]
                im = [field[ry, pl.ds(k * m + base, half), m:] for k in range(radix)]
                for rx, parts in enumerate(radix4(re, im)):
                    for p, part in enumerate(parts):
                        hi, lo = split(part)
                        cols[rx, pl.ds(p * m + base, half), ry * m:(ry + 1) * m] = hi
                        cols[rx, pl.ds((2 + p) * m + base, half), ry * m:(ry + 1) * m] = lo

        for rx in range(radix):
            hi, lo = cols[rx, :2 * m], cols[rx, 2 * m:]
            th, tl = colt[rx, :, :2 * m], colt[rx, :, 2 * m:]
            done = jnp.dot(jnp.concatenate([th, th, tl], 1), jnp.concatenate([hi, lo, hi], 0),
                           preferred_element_type=F32)
            power = (done[:m] * done[:m] + done[m:] * done[m:]) * weight_ref[s]
            if s == 0:
                total[rx] = power
            else:
                total[rx] += power

    for s in range(steps):
        own = piece(s, g, z, y)
        for d in range(1, nz):
            send(own, own, z_send.at[s, d], z_recv.at[s, d], {"tile": 2 * near(d) + y})
        cross(s, 0)
    for load in loads[1:]:
        load.wait()
    gather_z(0)
    for s in range(steps):
        if s + 1 < steps:
            gather_z(s + 1)
        gather_xy(s)
        if s:
            compute(s - 1)
    compute(steps - 1)

    for rx in range(radix):
        hi, lo = split(total[rx])
        perm = lane_perm[...]
        image = jnp.dot(jnp.concatenate([hi, lo], 1), jnp.concatenate([perm, perm], 0), preferred_element_type=F32)
        for q in range(radix):
            blocks[q, pl.ds(rx, m, stride=radix), :] = image[:, q * m:(q + 1) * m]
    for q in range(radix):
        out_ref[:, q * m:(q + 1) * m] = blocks[q]
    for copy in sent:
        copy.wait_send()


def local(mesh_shape, mask_spectrum, kernels, owner_table, step_weight):
    groups, tiles = mesh_shape
    nk, _, rows, n = kernels.shape
    steps = owner_table.shape[0]
    m = n // groups
    radix = groups
    nz = tiles // 2
    rowt, colt = tables(n, radix)
    dma = pltpu.SemaphoreType.DMA
    any_spec = pl.BlockSpec(memory_space=pl.ANY)
    smem = pl.BlockSpec(memory_space=pltpu.SMEM)
    out = pl.pallas_call(
        functools.partial(kernel, (steps, groups, nk, nz, rows, n, m)),
        out_shape=jax.ShapeDtypeStruct((n, n), F32),
        in_specs=[smem, smem, any_spec, any_spec, any_spec, any_spec],
        out_specs=pl.BlockSpec(memory_space=pltpu.VMEM),
        scratch_shapes=[
            pltpu.VMEM((steps, groups, 2, nz, 2, rows, m), F32),
            pltpu.VMEM((groups * nk, 2, rows, m), F32),
            pltpu.VMEM((2, n, n), F32),
            pltpu.VMEM(rowt.shape, BF),
            pltpu.VMEM(colt.shape, BF),
            pltpu.VMEM((n, n), BF),
            pltpu.VMEM((radix, n, 4 * m), BF),
            pltpu.VMEM((radix, n, 2 * m), F32),
            pltpu.VMEM((radix, 4 * m, n), BF),
            pltpu.VMEM((radix, m, n), F32),
            pltpu.VMEM((radix, n, m), F32),
        ] + [dma((steps, nz))] * 8 + [dma((steps, 4))] * 2 + [dma((groups - 1,))] * 2 + [dma((4,))],
        compiler_params=pltpu.CompilerParams(collective_id=0, has_side_effects=True, vmem_limit_bytes=62 * 1024 * 1024),
    )(owner_table, step_weight, mask_spectrum[0], kernels, jnp.asarray(rowt), jnp.asarray(colt))
    return out[None]


def solution(mesh):
    in_specs = (P(("kgrp", "tile"), None, None, None), P("kgrp", None, "tile", None), P(), P())
    out_specs = P(("kgrp", "tile"), None, None)
    body = functools.partial(local, (mesh.shape["kgrp"], mesh.shape["tile"]))
    return jax.shard_map(body, mesh=mesh, in_specs=in_specs, out_specs=out_specs, check_vma=False)
```
